32 devices in a mesh: trow: 4 (over y, x), tcol: 4 (over z), dp: 2 (over core).
Axes of the slice: x: 2, y: 2, z: 4, core: 2. Of those that a mesh axis runs over, the one named last changes fastest.
Arguments:
- embeds: bfloat16 [2048, 1024], P('dp'), may hold values from -6 to 6
- frequencies: bfloat16 [1024, 8192], P(None, ('trow', 'tcol')), may hold values from -0.5 to 0.5
- phases: float32 [8192], P(('trow', 'tcol')), may hold values from -3.140625 to 3.140625
- labels: int32 [2048], P('dp'), may hold values from 0 to 999
- weights: float32 [8192, 1000], P(('tcol', 'dp'), 'trow'), may hold values from -6 to 6
Outputs:
- gram_matrix: float32 [8192, 8192], P(('trow', 'dp'), 'tcol')
- new_weights: float32 [8192, 1000], P(('tcol', 'dp'), 'trow')
The draws below stay inside these ranges and needn't reach their ends.
All inputs are finite; a program needn't handle non-finite values.
Results may differ from the reference program's by a relative error of at most 0.023.
Values may be sent and summed in bfloat16 or wider, within the bound.
No kernel may reach another device: no remote copies, remote signals or barrier semaphores. Data moves between devices by JAX's collectives and lax.ppermute only.
A program may use at most 128 MiB of HBM per device.

```python
import jax
import jax.numpy as jnp
from jax import lax

DIN = 1024
F = 8192
C = 1000
ROWS_DEV = 1024
ROWS = 2048
N_DP = 2


def with_ends(array, own_key, smallest, largest):
    place = [jax.random.randint(jax.random.fold_in(own_key, axis), (), 0, length) for axis, length in enumerate(array.shape)]
    widest = array.shape.index(max(array.shape))
    next_to = place[:widest] + [(place[widest] + 1) % array.shape[widest]] + place[widest + 1:]
    return array.at[tuple(place)].set(smallest).at[tuple(next_to)].set(largest)


def steps_of(rng, extent, split, smallest, top_value):
    level, own = 1.0, jax.random.fold_in(rng, 6)
    for position, blocks in split:
        steps = jnp.exp(jax.random.uniform(jax.random.fold_in(own, position), (blocks,), jnp.float32, smallest / len(split), top_value / len(split)))
        level = level * jnp.repeat(steps, extent[position] // blocks).reshape([-1 if axis == position else 1 for axis in range(len(extent))])
    return level


def scatter_about(stream_key, dims, deviation, most, shards=(), kind=jnp.bfloat16):
    gain = steps_of(stream_key, dims, shards, -0.22, 0.18) if shards else 1.0
    values = jax.random.normal(stream_key, dims, jnp.float32) * deviation * gain
    return jnp.minimum(jnp.maximum(values, -most), most).astype(kind)


def setup_inputs(seed: int = 0) -> dict:
    seeds = jax.random.split(jax.random.key(seed), 6)
    return {
        "embeds": scatter_about(seeds[0], (ROWS, DIN), 1.0, 6.0, ((0, 2),)),
        "frequencies": scatter_about(seeds[1], (DIN, F), (DIN // 9) ** -0.5, 0.5, ((1, 16),)),
        "phases": jnp.clip(jax.random.uniform(seeds[2], (F,), jnp.float32, -3.140625, 3.140625), -3.140625, 3.140625),
        "labels": with_ends(jax.random.randint(seeds[3], (ROWS,), 0, C), jax.random.fold_in(seeds[3], 1), 0, C - 1).astype(jnp.int32),
        "weights": scatter_about(seeds[4], (F, C), 1.0, 6.0, ((0, 8), (1, 4)), jnp.float32),
    }


ROOT_TWO = 1.4142135623730951
RIDGE = 0.5
STEP_RATE = 0.5


def featurize(embeds, frequencies, phases):
    angles = jnp.dot(embeds, frequencies, preferred_element_type=jnp.float32) + phases
    return (ROOT_TWO * jnp.cos(angles)).astype(jnp.bfloat16)


def rounded(values):
    return lax.optimization_barrier(values.astype(jnp.bfloat16)).astype(jnp.float32)


def reference(embeds, frequencies, phases, labels, weights):
    features = featurize(embeds, frequencies, phases)
    grouped = features.reshape(N_DP, ROWS_DEV, F)
    group_labels = labels.reshape(N_DP, ROWS_DEV)
    class_ids = jnp.arange(C, dtype=jnp.int32)
    contract = (((0,), (0,)), ((), ()))

    def accumulate(carry, group_item):
        gram_sum, label_sum = carry
        group_rows, labels_here = group_item
        wide_rows = group_rows.astype(jnp.float32)
        gram_part = lax.dot_general(wide_rows, wide_rows, contract, precision=lax.Precision.HIGHEST) / ROWS
        onehot = (labels_here[:, None] == class_ids[None, :]).astype(jnp.float32)
        label_part = lax.dot_general(wide_rows, onehot, contract, precision=lax.Precision.HIGHEST) * (C / ROWS)
        return (gram_sum + rounded(gram_part), label_sum + rounded(label_part)), None

    init = (jnp.zeros((F, F), jnp.float32), jnp.zeros((F, C), jnp.float32))
    (gram_sum, label_sum), unused = lax.scan(accumulate, init, (grouped, group_labels))
    gram_matrix = gram_sum + RIDGE * jnp.eye(F, dtype=jnp.float32)
    curvature = jnp.dot(rounded(gram_matrix), rounded(weights), precision=lax.Precision.HIGHEST)
    diag_vals = jnp.diagonal(gram_matrix)
    new_weights = weights - STEP_RATE * (curvature - label_sum) / diag_vals[:, None]
    return gram_matrix, new_weights
```

```python
import jax
import jax.numpy as jnp
from jax import lax
from jax.sharding import PartitionSpec as P


RIDGE = 0.5
STEP_RATE = 0.5
INV_TWO_PI = 0.15915494309189535
COS_POLY = (
    1.4142135469,
    -27.9154507136,
    91.8377806403,
    -120.844746231,
    85.0898797067,
    -36.7237310395,
    9.23291691607,
)
CONTRACT = (((0,), (0,)), ((), ()))


def cosine(angles):
    turns = angles * INV_TWO_PI
    turns = turns - jnp.round(turns)
    square = turns * turns
    value = jnp.full_like(square, COS_POLY[-1])
    for coef in COS_POLY[-2::-1]:
        value = value * square + coef
    return value.astype(jnp.bfloat16)


def featurize(rows, freqs, phases):
    return cosine(jnp.dot(rows, freqs, preferred_element_type=jnp.float32) + phases)


def contract(left, right):
    return lax.dot_general(left, right, CONTRACT, preferred_element_type=jnp.float32)


def shift(array, axis, by):
    size = lax.axis_size(axis)
    return lax.ppermute(array, axis, [(i, (i + by) % size) for i in range(size)])


def swap(array, axis, bit):
    size = lax.axis_size(axis)
    return lax.ppermute(array, axis, [(i, i ^ bit) for i in range(size)])


def pick(array, index, size):
    return lax.dynamic_slice_in_dim(array, index * size, size, 0)


def roll_blocks(blocks, start):
    rows = blocks[0].shape[0]
    return lax.dynamic_slice_in_dim(
        jnp.concatenate(blocks + blocks[:-1], 0), start * rows, rows * len(blocks), 0
    )


def two_core(embeds, frequencies, phases, labels, weights):
    n = lax.axis_size("trow")
    row_idx = lax.axis_index("trow")
    col_idx = lax.axis_index("tcol")
    dp_idx = lax.axis_index("dp")
    rows_here, din = embeds.shape
    total_rows = 2 * rows_here
    width = frequencies.shape[1]
    class_width = weights.shape[1]
    half_din, part = din // 2, din // 2 // n

    own_half = pick(frequencies, dp_idx, half_din)
    pieces = own_half.reshape(n, part, width)

    def piece_of(stack, index):
        return lax.dynamic_index_in_dim(stack, index, 0, keepdims=False)

    with_row = [
        piece_of(pieces, row_idx) if k == 0 else swap(piece_of(pieces, row_idx ^ k), "trow", k)
        for k in range(n)
    ]
    left_slots = [own_half] + [shift(own_half, "tcol", s) for s in range(1, n)]
    emb_peer = swap(embeds, "dp", 1)
    low_weights = weights.astype(jnp.bfloat16)
    weights_peer = swap(low_weights, "dp", 1)
    all_phases = lax.all_gather(phases, ("trow", "tcol"), axis=0, tiled=False)

    row_stack = jnp.stack(with_row)
    by_plane = []
    for s in range(n):
        to_plane = (col_idx + s) % n
        piece = piece_of(row_stack, row_idx ^ to_plane)
        by_plane.append(piece if s == 0 else shift(piece, "tcol", s))

    emb_all = jnp.concatenate([embeds, emb_peer], 0)
    halves = [pick(emb_all.T, dp_idx, half_din).T, pick(emb_all.T, 1 - dp_idx, half_din).T]
    emb_left = jnp.concatenate(halves, 1)
    emb_right = jnp.concatenate(
        [lax.dynamic_slice_in_dim(h, (row_idx ^ k) * part, part, 1) for h in halves for k in range(n)], 1
    )

    right = []
    for s in range(n):
        quarters = [by_plane[s]] + [swap(by_plane[s], "trow", k) for k in range(1, n)]
        mine = jnp.concatenate(quarters, 0)
        block = jnp.concatenate([mine, swap(mine, "dp", 1)], 0)
        ph = all_phases[col_idx * n + (col_idx - s) % n]
        right.append(featurize(emb_right, block, ph))

    ordered = jnp.where(dp_idx == 0, jnp.concatenate([low_weights, weights_peer], 0), jnp.concatenate([weights_peer, low_weights], 0))
    scores = sum(
        jnp.dot(right[s][:rows_here], pick(ordered, (col_idx - s) % n, width), preferred_element_type=jnp.float32)
        for s in range(n)
    ).astype(jnp.bfloat16)
    quarter = rows_here // n
    total = pick(scores, col_idx, quarter).astype(jnp.float32)
    for s in range(1, n):
        total = total + shift(pick(scores, (col_idx + s) % n, quarter), "tcol", s).astype(jnp.float32)
    class_ids = row_idx * class_width + jnp.arange(class_width, dtype=jnp.int32)
    hot = (pick(labels, col_idx, quarter)[:, None] == class_ids[None, :]).astype(jnp.float32)
    resid = (total - (class_width * n) * hot).astype(jnp.bfloat16)
    around = [resid] + [shift(resid, "tcol", n - t) for t in range(1, n)]
    resid_own = roll_blocks(around, (n - col_idx) % n)
    resid_all = jnp.concatenate([resid_own, swap(resid_own, "dp", 1)], 0)

    per_core = n // 2
    left_stack = jnp.stack(left_slots)

    def slot_of(index):
        return piece_of(left_stack, (col_idx - index) % n)

    keep = [slot_of(per_core * dp_idx + k) for k in range(per_core)]
    send = jnp.stack([slot_of(per_core * (1 - dp_idx) + k) for k in range(per_core)])
    came = swap(send, "dp", 1)
    left = []
    for k in range(per_core):
        block = jnp.concatenate([keep[k], came[k]], 0)
        ph = all_phases[row_idx * n + per_core * dp_idx + k]
        left.append(featurize(emb_left, block, ph))
    left = jnp.concatenate(left, 1)
    rows = per_core * width
    global_rows = (row_idx * n + per_core * dp_idx) * width + jnp.arange(rows, dtype=jnp.int32)
    gram = jnp.zeros((rows, n * width), jnp.float32)
    for s in range(n):
        at = (col_idx - s) % n
        cols = (col_idx * n + at) * width + jnp.arange(width, dtype=jnp.int32)
        tile = contract(left, right[s]) / total_rows
        tile = tile + RIDGE * (global_rows[:, None] == cols[None, :]).astype(jnp.float32)
        gram = lax.dynamic_update_slice_in_dim(gram, tile, at * width, 1)

    grads, norms = [], []
    for s in range(n):
        wide = right[s].astype(jnp.float32)
        norms.append(jnp.sum(wide * wide, 0))
        grads.append(contract(right[s], resid_all))

    def own_rows(parts):
        order = [parts[0]] + [parts[n - t] for t in range(1, n)]
        natural = roll_blocks(order, (n - col_idx) % n)
        return pick(natural, dp_idx, rows)

    grad = own_rows(grads) / total_rows + RIDGE * weights
    diag = own_rows(norms) / total_rows + RIDGE
    return gram, weights - STEP_RATE * grad / diag[:, None]


def many_core(embeds, frequencies, phases, labels, weights):
    n_dp = lax.axis_size("dp")
    row_idx = lax.axis_index("trow")
    col_idx = lax.axis_index("tcol")
    dp_idx = lax.axis_index("dp")
    total_rows = embeds.shape[0] * n_dp
    own = featurize(embeds, frequencies, phases)
    left = lax.all_gather(own, "tcol", axis=1, tiled=True)
    right = lax.psum(jnp.where(row_idx == col_idx, left, jnp.zeros_like(left)), "trow")
    tile_width = left.shape[1]
    sub_rows = tile_width // n_dp
    gram = lax.psum_scatter(
        (contract(left, right) / total_rows).astype(jnp.bfloat16), "dp", scatter_dimension=0, tiled=True
    ).astype(jnp.float32)
    global_rows = row_idx * tile_width + dp_idx * sub_rows + jnp.arange(sub_rows, dtype=jnp.int32)
    global_cols = col_idx * tile_width + jnp.arange(tile_width, dtype=jnp.int32)
    gram = gram + RIDGE * (global_rows[:, None] == global_cols[None, :]).astype(jnp.float32)
    col_weights = lax.all_gather(weights.astype(jnp.bfloat16), "dp", axis=0, tiled=True)
    class_width = weights.shape[1]
    scores = lax.psum(jnp.dot(right, col_weights, preferred_element_type=jnp.float32), "tcol")
    class_ids = row_idx * class_width + jnp.arange(class_width, dtype=jnp.int32)
    hot = (labels[:, None] == class_ids[None, :]).astype(jnp.float32)
    resid = (scores - (class_width * lax.axis_size("trow")) * hot).astype(jnp.bfloat16)
    grad = lax.psum_scatter(contract(right, resid), "dp", scatter_dimension=0, tiled=True)
    wide = right.astype(jnp.float32)
    norm = lax.psum_scatter(jnp.sum(wide * wide, 0), "dp", scatter_dimension=0, tiled=True)
    grad = grad / total_rows + RIDGE * weights
    diag = norm / total_rows + RIDGE
    return gram, weights - STEP_RATE * grad / diag[:, None]


def solution(mesh):
    n, m, cores = mesh.shape["trow"], mesh.shape["tcol"], mesh.shape["dp"]
    body = two_core if n == m and cores == 2 and n & (n - 1) == 0 else many_core
    return jax.shard_map(
        body,
        mesh=mesh,
        in_specs=(
            P("dp", None),
            P(None, ("trow", "tcol")),
            P(("trow", "tcol")),
            P("dp"),
            P(("tcol", "dp"), "trow"),
        ),
        out_specs=(P(("trow", "dp"), "tcol"), P(("tcol", "dp"), "trow")),
        check_vma=False,
    )
```

```python
import jax
import jax.numpy as jnp
from jax import lax
from jax.experimental import pallas as pl
from jax.experimental.pallas import tpu as pltpu
from jax.sharding import PartitionSpec as P


RIDGE = 0.5
STEP_RATE = 0.5
INV_TWO_PI = 0.15915494309189535
COS_POLY = (
    1.4142135469,
    -27.9154507136,
    91.8377806403,
    -120.844746231,
    85.0898797067,
    -36.7237310395,
    9.23291691607,
)
CONTRACT = (((0,), (0,)), ((), ()))


def cosine(angles):
    turns = angles * INV_TWO_PI
    turns = turns - jnp.round(turns)
    square = turns * turns
    value = jnp.full_like(square, COS_POLY[-1])
    for coef in COS_POLY[-2::-1]:
        value = value * square + coef
    return value.astype(jnp.bfloat16)


def featurize(rows, freqs, phases):
    return cosine(jnp.dot(rows, freqs, preferred_element_type=jnp.float32) + phases)


def contract(left, right):
    return lax.dot_general(left, right, CONTRACT, preferred_element_type=jnp.float32)


def swap(array, axis, bit):
    size = lax.axis_size(axis)
    return lax.ppermute(array, axis, [(i, i ^ bit) for i in range(size)])


def pick(array, index, size):
    return lax.dynamic_slice_in_dim(array, index * size, size, 0)


TAIL = 16


def join_phases(tail):
    wide = tail.astype(jnp.float32)
    return wide[0:1] + (wide[1:2] + wide[2:3])


def prepare_kernel(n, idx, freq, phases, *outs):
    part = freq.shape[0] // 2 // n
    value = phases[...]
    high = value.astype(jnp.bfloat16).astype(jnp.float32)
    rest = value - high
    mid = rest.astype(jnp.bfloat16).astype(jnp.float32)
    low = rest - mid
    row = lax.broadcasted_iota(jnp.int32, (TAIL, freq.shape[1]), 0)
    tail = jnp.where(row == 0, high, jnp.where(row == 1, mid, jnp.where(row == 2, low, 0.0)))
    tail = tail.astype(jnp.bfloat16)
    packed = outs[n]
    for k in range(n):
        start = pl.multiple_of(idx[2] * (part * n) + (idx[1] ^ k) * part, part)
        piece = freq[pl.ds(start, part), :]
        outs[k][:part, :] = piece
        outs[k][part:, :] = tail
        packed[k * part : (k + 1) * part, :] = piece
    packed[n * part :, :] = tail


def prepare(n, idx, freq, phases):
    din, width = freq.shape
    part = din // 2 // n
    shapes = [(part + TAIL, width)] * n + [(n * part + TAIL, width)]
    vmem = pl.BlockSpec(memory_space=pltpu.VMEM)
    return pl.pallas_call(
        lambda *refs: prepare_kernel(n, *refs),
        out_shape=[jax.ShapeDtypeStruct(shape, jnp.bfloat16) for shape in shapes],
        in_specs=[pl.BlockSpec(memory_space=pltpu.SMEM), vmem, vmem],
        out_specs=[vmem] * (n + 1),
        name="prepare",
    )(idx, freq, phases[None])


def arrange_kernel(n, idx, rows, out):
    part = rows.shape[1] // 2 // n
    for h in range(2):
        for k in range(n):
            start = pl.multiple_of((idx[2] ^ h) * (part * n) + (idx[1] ^ k) * part, part)
            at = (h * n + k) * part
            out[:, at : at + part] = rows[:, pl.ds(start, part)]


def arrange(n, idx, rows):
    count, din = rows.shape
    quarter = count // n
    return pl.pallas_call(
        lambda *refs: arrange_kernel(n, *refs),
        out_shape=jax.ShapeDtypeStruct((count, din), rows.dtype),
        grid_spec=pltpu.PrefetchScalarGridSpec(
            num_scalar_prefetch=1,
            grid=(n,),
            in_specs=[pl.BlockSpec((quarter, din), lambda i, idx: (idx[0] ^ i, 0))],
            out_specs=pl.BlockSpec((quarter, din), lambda i, idx: (i, 0)),
        ),
        name="arrange",
    )(idx, rows)


def send(array, axis, pairs):
    return lax.ppermute(array, axis, pairs)


def two_core(*args):
    return two_core_body(*args)


def two_core_body(embeds, frequencies, phases, labels, weights):
    n = lax.axis_size("trow")
    row_idx = lax.axis_index("trow")
    col_idx = lax.axis_index("tcol")
    dp_idx = lax.axis_index("dp")
    idx = jnp.stack([col_idx, row_idx, dp_idx]).astype(jnp.int32)
    rows_here, din = embeds.shape
    total_rows = 2 * rows_here
    width = frequencies.shape[1]
    class_width = weights.shape[1]
    half_din, part = din // 2, din // 2 // n
    quarter = rows_here // n
    per_core = n // 2
    others = range(1, n)

    *pieces, packed = prepare(n, idx, frequencies, phases)

    with_row = [pieces[0]]
    for k in others:
        with_row.append(swap(pieces[k], "trow", k))
    near = swap(packed, "tcol", 1)
    mid = send(packed, "tcol", [(1, 2), (2, 1)])
    emb_peer = swap(embeds, "dp", 1)
    emb_own = arrange(n, idx, embeds)
    emb_peer = arrange(n, idx, emb_peer)

    by_plane = []
    for s in range(n):
        piece = lax.select_n(row_idx ^ col_idx ^ s, *with_row)
        by_plane.append(piece if s == 0 else swap(piece, "tcol", s))
    weights_later, *unused = lax.optimization_barrier((weights, *with_row))
    low_weights = weights_later.astype(jnp.bfloat16)
    weights_peer = swap(low_weights, "dp", 1)
    near_later, mid_later, *unused = lax.optimization_barrier((near, mid, *by_plane))
    across = send(near_later, "tcol", [(1, 2), (2, 1)])
    out = send(mid_later, "tcol", [(1, 0), (2, 3)])
    last = send(across, "tcol", [(1, 0), (2, 3)])
    inner = (col_idx == 1) | (col_idx == 2)
    left_slots = [packed, near, jnp.where(inner, across, out), jnp.where(inner, mid, last)]

    def gathered(piece):
        mine = [piece]
        for k in others:
            mine.append(swap(piece, "trow", k))
        mine = jnp.concatenate(mine, 0)
        other = swap(mine, "dp", 1)
        return jnp.concatenate([mine, other], 0)

    def both(block, tail):
        phase = join_phases(tail)
        own = featurize(emb_own, block, phase)
        peer = featurize(emb_peer, block, phase)
        return own, peer

    first = gathered(by_plane[0][:part])
    first_own, first_peer = both(first, by_plane[0][part:])
    rest_pieces = jnp.concatenate(by_plane[1:], 1)
    rest = gathered(rest_pieces[:part])
    rest_own, rest_peer = both(rest, rest_pieces[part:])

    stacked = jnp.stack([low_weights, weights_peer]).reshape(n, width, class_width)

    def weights_of(s):
        return lax.dynamic_index_in_dim(stacked, col_idx ^ s ^ (dp_idx * per_core), 0, keepdims=False)

    rest_weights = jnp.concatenate([weights_of(s) for s in others], 0)
    scores = jnp.dot(first_own, weights_of(0), preferred_element_type=jnp.float32)
    scores = scores + jnp.dot(rest_own, rest_weights, preferred_element_type=jnp.float32)
    scores = scores.astype(jnp.bfloat16)
    total = scores[:quarter].astype(jnp.float32)
    for s in others:
        came = swap(scores[s * quarter : (s + 1) * quarter], "tcol", s)
        total = total + came.astype(jnp.float32)
    class_ids = row_idx * class_width + jnp.arange(class_width, dtype=jnp.int32)
    hot = (pick(labels, col_idx, quarter)[:, None] == class_ids[None, :]).astype(jnp.float32)
    resid = (total - (class_width * n) * hot).astype(jnp.bfloat16)
    around = []
    for k in others:
        around.append(swap(resid, "tcol", k))

    left_slots, unused = lax.optimization_barrier((left_slots, scores))
    left_stack = jnp.stack(left_slots)

    def slot_of(index):
        return lax.dynamic_index_in_dim(left_stack, col_idx ^ index, 0, keepdims=False)

    keep = jnp.concatenate([slot_of(per_core * dp_idx + k) for k in range(per_core)], 1)
    give = jnp.concatenate([slot_of(per_core * (1 - dp_idx) + k) for k in range(per_core)], 1)
    other = swap(give[:half_din], "dp", 1)
    left_own, left_peer = both(jnp.concatenate([keep[:half_din], other], 0), keep[half_din:])
    resid = jnp.concatenate([resid, *around], 0)
    resid_peer = swap(resid, "dp", 1)
    rows = per_core * width
    global_rows = (row_idx * n + per_core * dp_idx) * width + jnp.arange(rows, dtype=jnp.int32)
    gram = jnp.zeros((rows, n * width), jnp.float32)
    for s in range(n):
        at = col_idx ^ s
        cols = (col_idx * n + at) * width + jnp.arange(width, dtype=jnp.int32)
        own, peer = [
            whole if s == 0 else part_[:, (s - 1) * width : s * width]
            for whole, part_ in ((first_own, rest_own), (first_peer, rest_peer))
        ]
        tile = (contract(left_own, own) + contract(left_peer, peer)) / total_rows
        tile = tile + RIDGE * (global_rows[:, None] == cols[None, :]).astype(jnp.float32)
        gram = lax.dynamic_update_slice_in_dim(gram, tile, at * width, 1)

    def own_cols(first_part, rest_part):
        cols = []
        for k in range(per_core):
            slot = col_idx ^ (per_core * dp_idx + k)
            found = lax.dynamic_slice_in_dim(rest_part, jnp.maximum(slot - 1, 0) * width, width, 1)
            cols.append(jnp.where(slot == 0, first_part, found))
        return jnp.concatenate(cols, 1)

    kept = (first_own, rest_own, first_peer, rest_peer)
    (first_own, rest_own, first_peer, rest_peer), unused = lax.optimization_barrier((kept, total))
    sel_own, sel_peer = own_cols(first_own, rest_own), own_cols(first_peer, rest_peer)
    norm = 0.0
    for selected in (sel_own, sel_peer):
        wide = selected.astype(jnp.float32)
        norm = norm + jnp.sum(wide * wide, 0)
    diag = norm / total_rows + RIDGE
    grad = (contract(sel_own, resid) + contract(sel_peer, resid_peer)) / total_rows + RIDGE * weights
    return gram, weights - STEP_RATE * grad / diag[:, None]


def many_core(embeds, frequencies, phases, labels, weights):
    n_dp = lax.axis_size("dp")
    row_idx = lax.axis_index("trow")
    col_idx = lax.axis_index("tcol")
    dp_idx = lax.axis_index("dp")
    total_rows = embeds.shape[0] * n_dp
    own = featurize(embeds, frequencies, phases)
    left = lax.all_gather(own, "tcol", axis=1, tiled=True)
    right = lax.psum(jnp.where(row_idx == col_idx, left, jnp.zeros_like(left)), "trow")
    tile_width = left.shape[1]
    sub_rows = tile_width // n_dp
    gram = lax.psum_scatter(
        (contract(left, right) / total_rows).astype(jnp.bfloat16), "dp", scatter_dimension=0, tiled=True
    ).astype(jnp.float32)
    global_rows = row_idx * tile_width + dp_idx * sub_rows + jnp.arange(sub_rows, dtype=jnp.int32)
    global_cols = col_idx * tile_width + jnp.arange(tile_width, dtype=jnp.int32)
    gram = gram + RIDGE * (global_rows[:, None] == global_cols[None, :]).astype(jnp.float32)
    col_weights = lax.all_gather(weights.astype(jnp.bfloat16), "dp", axis=0, tiled=True)
    class_width = weights.shape[1]
    scores = lax.psum(jnp.dot(right, col_weights, preferred_element_type=jnp.float32), "tcol")
    class_ids = row_idx * class_width + jnp.arange(class_width, dtype=jnp.int32)
    hot = (labels[:, None] == class_ids[None, :]).astype(jnp.float32)
    resid = (scores - (class_width * lax.axis_size("trow")) * hot).astype(jnp.bfloat16)
    grad = lax.psum_scatter(contract(right, resid), "dp", scatter_dimension=0, tiled=True)
    wide = right.astype(jnp.float32)
    norm = lax.psum_scatter(jnp.sum(wide * wide, 0), "dp", scatter_dimension=0, tiled=True)
    grad = grad / total_rows + RIDGE * weights
    diag = norm / total_rows + RIDGE
    return gram, weights - STEP_RATE * grad / diag[:, None]


def solution(mesh):
    n, m, cores = mesh.shape["trow"], mesh.shape["tcol"], mesh.shape["dp"]
    small = n == m == 4 and cores == 2
    return jax.shard_map(
        two_core if small else many_core,
        mesh=mesh,
        in_specs=(
            P("dp", None),
            P(None, ("trow", "tcol")),
            P(("trow", "tcol")),
            P("dp"),
            P(("tcol", "dp"), "trow"),
        ),
        out_specs=(P(("trow", "dp"), "tcol"), P(("tcol", "dp"), "trow")),
        check_vma=False,
    )
```
